8 devices in a mesh: data: 8 (over z, y, x, core).
Axes of the slice: x: 2, y: 2, z: 1, core: 2. Of those that a mesh axis runs over, the one named last changes fastest.
Arguments:
- feat_a: bfloat16 [8192, 2048], P('data')
- feat_b: bfloat16 [8192, 2048], P('data')
- w_in: bfloat16 [2048, 4096], replicated
- w_mid: bfloat16 [4096, 4096], replicated
- w_out: bfloat16 [4096, 4096], replicated
- t_in: bfloat16 [2048, 4096], replicated
- t_mid: bfloat16 [4096, 4096], replicated
- t_out: bfloat16 [4096, 4096], replicated
- gain_1: float32 [4096], replicated
- bias_1: float32 [4096], replicated
- gain_2: float32 [4096], replicated
- bias_2: float32 [4096], replicated
- off_weight: float32 [], replicated
Outputs:
- output 1: float32 [], replicated
- output 2: float32 [8192, 4096], P('data')
- output 3: float32 [2048, 4096], replicated
- output 4: float32 [4096, 4096], replicated
- output 5: float32 [4096, 4096], replicated
- output 6: float32 [4096], replicated
- output 7: float32 [4096], replicated
- output 8: float32 [4096], replicated
- output 9: float32 [4096], replicated
All inputs are finite; a program needn't handle non-finite values.
Results may differ from the reference program's by a relative error of at most 0.00515.
Values are sent between devices in bfloat16 or wider.
A program may use at most 1.5 GiB of HBM per device.

```python
import jax
import jax.numpy as jnp
from jax import lax

FEAT_DIM = 2048
PROJ_DIM = 4096
ROWS_DEV = 1024
SHARDS = 8
ROWS = ROWS_DEV * SHARDS
NORM_EPS = 1e-5


def setup_inputs(seed: int = 0) -> dict:
    key_list = jax.random.split(jax.random.key(seed), 16)
    row_shape = (SHARDS, ROWS_DEV, FEAT_DIM)
    base_draw = jax.random.normal(key_list[0], row_shape, jnp.float32)
    view_noise = jax.random.normal(key_list[1], row_shape, jnp.float32)
    shard_shift = 0.5 * jax.random.normal(key_list[2], (SHARDS, 1, FEAT_DIM), jnp.float32)
    shard_scale = jax.random.uniform(key_list[3], (SHARDS, 1, FEAT_DIM), jnp.float32, 0.6, 1.4)
    feat_a = (base_draw * shard_scale + shard_shift).reshape(ROWS, FEAT_DIM)
    feat_b = ((0.8 * base_draw + 0.6 * view_noise) * shard_scale + shard_shift).reshape(ROWS, FEAT_DIM)
    in_scale = FEAT_DIM ** -0.5
    hid_scale = PROJ_DIM ** -0.5
    in_shape = (FEAT_DIM, PROJ_DIM)
    hid_shape = (PROJ_DIM, PROJ_DIM)
    w_in = in_scale * jax.random.normal(key_list[4], in_shape, jnp.float32)
    w_mid = hid_scale * jax.random.normal(key_list[5], hid_shape, jnp.float32)
    w_out = hid_scale * jax.random.normal(key_list[6], hid_shape, jnp.float32)
    t_in = 0.8 * w_in + 0.6 * in_scale * jax.random.normal(key_list[7], in_shape, jnp.float32)
    t_mid = 0.8 * w_mid + 0.6 * hid_scale * jax.random.normal(key_list[8], hid_shape, jnp.float32)
    t_out = 0.8 * w_out + 0.6 * hid_scale * jax.random.normal(key_list[9], hid_shape, jnp.float32)
    gain_1 = jax.random.uniform(key_list[10], (PROJ_DIM,), jnp.float32, 0.5, 1.5)
    bias_1 = 0.3 * jax.random.normal(key_list[11], (PROJ_DIM,), jnp.float32)
    gain_2 = jax.random.uniform(key_list[12], (PROJ_DIM,), jnp.float32, 0.5, 1.5)
    bias_2 = 0.3 * jax.random.normal(key_list[13], (PROJ_DIM,), jnp.float32)
    off_weight = (ROWS / PROJ_DIM) * jax.random.uniform(key_list[14], (), jnp.float32, 0.1, 0.3)
    return {
        "feat_a": feat_a.astype(jnp.bfloat16),
        "feat_b": feat_b.astype(jnp.bfloat16),
        "w_in": w_in.astype(jnp.bfloat16),
        "w_mid": w_mid.astype(jnp.bfloat16),
        "w_out": w_out.astype(jnp.bfloat16),
        "t_in": t_in.astype(jnp.bfloat16),
        "t_mid": t_mid.astype(jnp.bfloat16),
        "t_out": t_out.astype(jnp.bfloat16),
        "gain_1": gain_1,
        "bias_1": bias_1,
        "gain_2": gain_2,
        "bias_2": bias_2,
        "off_weight": off_weight,
    }


def batch_norm(pre_norm):
    mean_u = jnp.mean(pre_norm, axis=0)
    centered = pre_norm - mean_u
    inv_std = lax.rsqrt(jnp.mean(centered * centered, axis=0) + NORM_EPS)
    return centered * inv_std, inv_std


def hidden_layer(layer_in, weight, gain_vec, bias_vec):
    normed, inv_std = batch_norm(jnp.dot(layer_in, weight, preferred_element_type=jnp.float32))
    pre_act = normed * gain_vec + bias_vec
    return jnp.maximum(pre_act, 0.0).astype(jnp.bfloat16), normed, inv_std, pre_act > 0.0


def norm_back(grad_n, normed, inv_std):
    mean_g = jnp.mean(grad_n, axis=0)
    mean_gn = jnp.mean(grad_n * normed, axis=0)
    return (grad_n - mean_g - normed * mean_gn) * inv_std


def reference(feat_a, feat_b, w_in, w_mid, w_out, t_in, t_mid, t_out, gain_1, bias_1, gain_2, bias_2, off_weight):
    row_count = feat_a.shape[0]
    act_1, normed_1, inv_1, mask_1 = hidden_layer(feat_a, w_in, gain_1, bias_1)
    act_2, normed_2, inv_2, mask_2 = hidden_layer(act_1, w_mid, gain_2, bias_2)
    zh_a, inv_z = batch_norm(jnp.dot(act_2, w_out, preferred_element_type=jnp.float32))
    teach_1 = hidden_layer(feat_b, t_in, gain_1, bias_1)[0]
    teach_2 = hidden_layer(teach_1, t_mid, gain_2, bias_2)[0]
    zh_b = batch_norm(jnp.dot(teach_2, t_out, preferred_element_type=jnp.float32))[0]
    emb_a = zh_a.astype(jnp.bfloat16)
    emb_b = zh_b.astype(jnp.bfloat16)
    corr_mat = jnp.dot(emb_a.T, emb_b, preferred_element_type=jnp.float32) / row_count
    proj_width = corr_mat.shape[0]
    on_diag = jnp.arange(proj_width)[:, None] == jnp.arange(proj_width)[None, :]
    loss_value = jnp.sum(jnp.square(1.0 - jnp.diagonal(corr_mat))) + off_weight * jnp.sum(jnp.square(jnp.where(on_diag, 0.0, corr_mat)))
    grad_c = jnp.where(on_diag, -2.0 * (1.0 - corr_mat), 2.0 * off_weight * corr_mat).astype(jnp.bfloat16)
    grad_emb = jnp.dot(emb_b, grad_c.T, preferred_element_type=jnp.float32) / row_count
    grad_z = norm_back(grad_emb, zh_a, inv_z).astype(jnp.bfloat16)
    grad_w_out = jnp.dot(act_2.T, grad_z, preferred_element_type=jnp.float32)
    grad_pre_2 = jnp.where(mask_2, jnp.dot(grad_z, w_out.T, preferred_element_type=jnp.float32), 0.0)
    grad_gain_2 = jnp.sum(grad_pre_2 * normed_2, axis=0)
    grad_bias_2 = jnp.sum(grad_pre_2, axis=0)
    grad_u_2 = norm_back(grad_pre_2 * gain_2, normed_2, inv_2).astype(jnp.bfloat16)
    grad_w_mid = jnp.dot(act_1.T, grad_u_2, preferred_element_type=jnp.float32)
    grad_pre_1 = jnp.where(mask_1, jnp.dot(grad_u_2, w_mid.T, preferred_element_type=jnp.float32), 0.0)
    grad_gain_1 = jnp.sum(grad_pre_1 * normed_1, axis=0)
    grad_bias_1 = jnp.sum(grad_pre_1, axis=0)
    grad_u_1 = norm_back(grad_pre_1 * gain_1, normed_1, inv_1).astype(jnp.bfloat16)
    grad_w_in = jnp.dot(feat_a.T, grad_u_1, preferred_element_type=jnp.float32)
    return (loss_value, grad_emb, grad_w_in, grad_w_mid, grad_w_out, grad_gain_1, grad_bias_1, grad_gain_2, grad_bias_2)
```

```python
import jax
import jax.numpy as jnp
from jax import lax
from jax.sharding import PartitionSpec as P

NORM_EPS = 1e-5
DATA_AXIS = "data"
F32 = jnp.float32
BF16 = jnp.bfloat16


def dot(left_op, right_op, left_dim, right_dim):
    return lax.dot_general(left_op, right_op, (((left_dim,), (right_dim,)), ((), ())), preferred_element_type=F32)


def solution(mesh):
    shards = mesh.shape[DATA_AXIS]
    chips = shards // 2
    row_part = P(DATA_AXIS, None)
    replicated = P()
    pair_groups = [[2 * i, 2 * i + 1] for i in range(chips)]
    pair_perm = [(i, i ^ 1) for i in range(shards)]

    def local_step(feat_a, feat_b, w_in, w_mid, w_out, t_in, t_mid, t_out, gain_1, bias_1, gain_2, bias_2, off_weight):
        row_count = feat_a.shape[0] * shards
        width = w_mid.shape[0]
        half = width // 2
        block = width // shards
        dev = lax.axis_index(DATA_AXIS)
        core = dev % 2
        chip = dev // 2
        own_start = core * half
        other_start = (1 - core) * half

        def rows_of(array, start, size):
            return lax.dynamic_slice_in_dim(array, start, size, 0)

        def cols_of(array, start, size):
            return lax.dynamic_slice_in_dim(array, start, size, 1)

        def gather(array):
            return lax.all_gather(array, DATA_AXIS, axis=0, tiled=True)

        def pair_gather(array):
            return lax.all_gather(array, DATA_AXIS, axis=0, tiled=True, axis_index_groups=pair_groups)

        def norm_rows(pre):
            sums = lax.all_gather(jnp.stack([jnp.sum(pre, axis=0), jnp.sum(pre * pre, axis=0)]), DATA_AXIS)
            means = jnp.sum(sums, axis=0) / row_count
            inv = lax.rsqrt(jnp.maximum(means[1] - means[0] * means[0], 0.0) + NORM_EPS)
            return (pre - means[0]) * inv

        def teacher_layer(layer_in, weight, gain_vec, bias_vec):
            normed = norm_rows(jnp.dot(layer_in, weight, preferred_element_type=F32))
            return jnp.maximum(normed * gain_vec + bias_vec, 0.0).astype(BF16)

        def stats(pre):
            mean = jnp.sum(pre, axis=1, keepdims=True) / row_count
            square = jnp.sum(pre * pre, axis=1, keepdims=True) / row_count
            return mean, lax.rsqrt(jnp.maximum(square - mean * mean, 0.0) + NORM_EPS)

        def norm_back(grad_n, normed, inv_std):
            mean_g = jnp.sum(grad_n, axis=1, keepdims=True) / row_count
            mean_gn = jnp.sum(grad_n * normed, axis=1, keepdims=True) / row_count
            return (grad_n - mean_g - normed * mean_gn) * inv_std

        def affine_back(grad_pre, normed, inv_std, gain_col):
            sum_gn = jnp.sum(grad_pre * normed, axis=1, keepdims=True)
            sum_g = jnp.sum(grad_pre, axis=1, keepdims=True)
            grad_u = (grad_pre - sum_g / row_count - normed * (sum_gn / row_count)) * (gain_col * inv_std)
            return grad_u.astype(BF16), jnp.concatenate([sum_gn, sum_g], axis=1)

        feat_all = gather(feat_a)
        teach_1 = teacher_layer(feat_b, t_in, gain_1, bias_1)
        teach_2 = teacher_layer(teach_1, t_mid, gain_2, bias_2)
        emb_b = norm_rows(jnp.dot(teach_2, t_out, preferred_element_type=F32)).astype(BF16)
        emb_b_all = gather(emb_b)

        gain_1h, bias_1h, gain_2h, bias_2h = (rows_of(v[:, None], own_start, half) for v in (gain_1, bias_1, gain_2, bias_2))

        pre_1 = dot(cols_of(w_in, own_start, half), feat_all, 0, 1)
        mean_1, inv_1 = stats(pre_1)
        act_1 = jnp.maximum((pre_1 - mean_1) * inv_1 * gain_1h + bias_1h, 0.0).astype(BF16)
        act_1_other = lax.ppermute(act_1, DATA_AXIS, pair_perm)

        w_mid_cols = cols_of(w_mid, own_start, half)
        pre_2 = dot(rows_of(w_mid_cols, own_start, half), act_1, 0, 0) + dot(rows_of(w_mid_cols, other_start, half), act_1_other, 0, 0)
        mean_2, inv_2 = stats(pre_2)
        act_2 = jnp.maximum((pre_2 - mean_2) * inv_2 * gain_2h + bias_2h, 0.0).astype(BF16)
        act_2_other = lax.ppermute(act_2, DATA_AXIS, pair_perm)

        w_out_cols = cols_of(w_out, dev * block, block)
        pre_z = dot(rows_of(w_out_cols, own_start, half), act_2, 0, 0) + dot(rows_of(w_out_cols, other_start, half), act_2_other, 0, 0)
        mean_z, inv_z = stats(pre_z)
        zh_a = (pre_z - mean_z) * inv_z
        emb_a = zh_a.astype(BF16)

        corr_mat = dot(emb_a, emb_b_all, 1, 0) / row_count
        on_diag = lax.broadcasted_iota(jnp.int32, corr_mat.shape, 0) + dev * block == lax.broadcasted_iota(jnp.int32, corr_mat.shape, 1)
        loss_part = jnp.sum(jnp.where(on_diag, jnp.square(1.0 - corr_mat), off_weight * jnp.square(corr_mat)))
        grad_c = jnp.where(on_diag, -2.0 * (1.0 - corr_mat), 2.0 * off_weight * corr_mat).astype(BF16)

        grad_z = norm_back(dot(grad_c, emb_b_all, 1, 1) / row_count, zh_a, inv_z).astype(BF16)
        grad_z_all = gather(grad_z)
        grad_emb = dot(emb_b, gather(grad_c), 1, 1) / row_count

        grad_w_out = pair_gather(dot(act_2, grad_z_all, 1, 1))
        normed_2 = (pre_2 - mean_2) * inv_2
        grad_pre_2 = jnp.where(normed_2 * gain_2h + bias_2h > 0.0, dot(rows_of(w_out, own_start, half), grad_z_all, 1, 0), 0.0)
        grad_u_2, affine_2 = affine_back(grad_pre_2, normed_2, inv_2, gain_2h)
        grad_u_2_all = pair_gather(grad_u_2)

        part_start = chip * block
        normed_1 = (rows_of(pre_1, part_start, block) - rows_of(mean_1, part_start, block)) * rows_of(inv_1, part_start, block)
        gain_1p, bias_1p = rows_of(gain_1h, part_start, block), rows_of(bias_1h, part_start, block)
        grad_pre_1 = jnp.where(normed_1 * gain_1p + bias_1p > 0.0, dot(rows_of(w_mid, own_start + part_start, block), grad_u_2_all, 1, 0), 0.0)
        grad_u_1, affine_1 = affine_back(grad_pre_1, normed_1, rows_of(inv_1, part_start, block), gain_1p)
        grad_w_in_parts = lax.all_gather(dot(feat_all, grad_u_1, 0, 1), DATA_AXIS)
        grad_w_mid = pair_gather(dot(act_1, grad_u_2_all, 1, 1))

        grad_w_in = grad_w_in_parts.reshape(chips, 2, -1, block).transpose(2, 1, 0, 3).reshape(-1, width)
        small = jnp.concatenate([affine_1, rows_of(affine_2, part_start, block)], axis=1).T
        small = jnp.concatenate([small, jnp.full((1, block), loss_part)], axis=0)
        small_all = lax.all_gather(small, DATA_AXIS)
        vectors = small_all.reshape(chips, 2, 5, block).transpose(2, 1, 0, 3).reshape(5, width)
        loss_value = jnp.sum(small_all[:, 4, 0])
        return (loss_value, grad_emb, grad_w_in, grad_w_mid, grad_w_out, vectors[0], vectors[1], vectors[2], vectors[3])

    return jax.shard_map(local_step, mesh=mesh, in_specs=(row_part, row_part) + (replicated,) * 11, out_specs=(replicated, row_part) + (replicated,) * 7, check_vma=False)
```

```python
import jax
import jax.numpy as jnp
from jax import lax
from jax.experimental import pallas as pl
from jax.experimental.layout import Layout, with_layout_constraint
from jax.experimental.pallas import tpu as pltpu
from jax.sharding import PartitionSpec as P

NORM_EPS = 1e-5
DATA_AXIS = "data"
F32 = jnp.float32
BF16 = jnp.bfloat16


barrier = lax.optimization_barrier


def dot(left_op, right_op, left_dim, right_dim):
    return lax.dot_general(left_op, right_op, (((left_dim,), (right_dim,)), ((), ())), preferred_element_type=F32)


def place_rows(buffer, pieces, starts, row_start, total_rows, total_cols, step=256):
    rows = pieces[0].shape[0]
    count = len(pieces)

    def kernel(where_ref, *refs):
        out_ref = refs[-1]
        for index in range(count):
            size = pieces[index].shape[1]
            if isinstance(starts[index], int):
                out_ref[:, starts[index]:starts[index] + size] = refs[index][...]
            else:
                out_ref[:, pl.ds(pl.multiple_of(where_ref[1 + index] * 128, 128), size)] = refs[index][...]

    where = jnp.stack([jnp.asarray(row_start // step, jnp.int32)] + [jnp.asarray(s // 128, jnp.int32) for s in starts])
    in_specs = [pl.BlockSpec((step, piece.shape[1]), lambda i, where_ref: (i, 0)) for piece in pieces]
    operands = list(pieces)
    aliases = {}
    if buffer is not None:
        in_specs.append(pl.BlockSpec(memory_space=pl.ANY))
        operands.append(buffer)
        aliases = {1 + count: 0}
    return pl.pallas_call(
        kernel,
        out_shape=jax.ShapeDtypeStruct((total_rows, total_cols), F32),
        grid_spec=pltpu.PrefetchScalarGridSpec(
            num_scalar_prefetch=1,
            grid=(rows // step,),
            in_specs=in_specs,
            out_specs=pl.BlockSpec((step, total_cols), lambda i, where_ref: (where_ref[0] + i, 0)),
        ),
        input_output_aliases=aliases,
        cost_estimate=pl.CostEstimate(flops=4 * 10**9, bytes_accessed=8 * rows * total_cols, transcendentals=0),
        compiler_params=pltpu.CompilerParams(vmem_limit_bytes=40 * 2**20),
    )(where, *operands)


def join_columns(parts, order, step=512):
    count, rows, cols = parts.shape

    def kernel(in_ref, out_ref):
        out_ref[...] = in_ref[0]

    return pl.pallas_call(
        kernel,
        out_shape=jax.ShapeDtypeStruct((rows, count * cols), F32),
        grid=(count, rows // step),
        in_specs=[pl.BlockSpec((1, step, cols), lambda i, j: (i, j, 0))],
        out_specs=pl.BlockSpec((step, cols), lambda i, j: (j, order(i))),
        cost_estimate=pl.CostEstimate(flops=4 * 10**9, bytes_accessed=8 * parts.size, transcendentals=0),
    )(parts)


def solution(mesh):
    shards = mesh.shape[DATA_AXIS]
    chips = shards // 2
    row_part = P(DATA_AXIS, None)
    replicated = P()
    pair_groups = [[2 * i, 2 * i + 1] for i in range(chips)]
    pair_perm = [(i, i ^ 1) for i in range(shards)]

    def local_step(feat_a, feat_b, w_in, w_mid, w_out, t_in, t_mid, t_out, gain_1, bias_1, gain_2, bias_2, off_weight):
        row_count = feat_a.shape[0] * shards
        width = w_mid.shape[0]
        half = width // 2
        block = width // shards
        dev = lax.axis_index(DATA_AXIS)
        core = dev % 2
        chip = dev // 2
        own_start = core * half
        other_start = (1 - core) * half

        def rows_of(array, start, size):
            return lax.dynamic_slice_in_dim(array, start, size, 0)

        def cols_of(array, start, size):
            return lax.dynamic_slice_in_dim(array, start, size, 1)

        def gather(array):
            return lax.all_gather(array, DATA_AXIS, axis=0, tiled=True)

        def pair_gather(array):
            return lax.all_gather(array, DATA_AXIS, axis=0, tiled=True, axis_index_groups=pair_groups)

        def norm_rows(pre):
            sums = lax.all_gather(jnp.stack([jnp.sum(pre, axis=0), jnp.sum(pre * pre, axis=0)]), DATA_AXIS)
            means = jnp.sum(sums, axis=0) / row_count
            inv = lax.rsqrt(jnp.maximum(means[1] - means[0] * means[0], 0.0) + NORM_EPS)
            return (pre - means[0]) * inv

        def teacher_layer(layer_in, weight, gain_vec, bias_vec):
            normed = norm_rows(jnp.dot(layer_in, weight, preferred_element_type=F32))
            return jnp.maximum(normed * gain_vec + bias_vec, 0.0).astype(BF16)

        def stats(pre):
            mean = jnp.sum(pre, axis=1, keepdims=True) / row_count
            square = jnp.sum(pre * pre, axis=1, keepdims=True) / row_count
            return mean, lax.rsqrt(jnp.maximum(square - mean * mean, 0.0) + NORM_EPS)

        def norm_back(grad_n, normed, inv_std):
            mean_g = jnp.sum(grad_n, axis=1, keepdims=True) / row_count
            mean_gn = jnp.sum(grad_n * normed, axis=1, keepdims=True) / row_count
            return (grad_n - mean_g - normed * mean_gn) * inv_std

        def affine_back(grad_pre, normed, inv_std, gain_col):
            sum_gn = jnp.sum(grad_pre * normed, axis=1, keepdims=True)
            sum_g = jnp.sum(grad_pre, axis=1, keepdims=True)
            grad_u = (grad_pre - sum_g / row_count - normed * (sum_gn / row_count)) * (gain_col * inv_std)
            return grad_u.astype(BF16), jnp.concatenate([sum_gn, sum_g], axis=1)

        feat_all = gather(feat_a)
        teach_1 = teacher_layer(feat_b, t_in, gain_1, bias_1)
        teach_2 = teacher_layer(teach_1, t_mid, gain_2, bias_2)
        emb_b = norm_rows(jnp.dot(teach_2, t_out, preferred_element_type=F32)).astype(BF16)
        emb_b_all = gather(emb_b)

        gain_1h, bias_1h, gain_2h, bias_2h = (rows_of(v[:, None], own_start, half) for v in (gain_1, bias_1, gain_2, bias_2))

        pre_1 = dot(cols_of(w_in, own_start, half), feat_all, 0, 1)
        mean_1, inv_1 = stats(pre_1)
        act_1 = jnp.maximum((pre_1 - mean_1) * inv_1 * gain_1h + bias_1h, 0.0).astype(BF16)
        act_1_other = lax.ppermute(act_1, DATA_AXIS, pair_perm)

        w_mid_cols = cols_of(w_mid, own_start, half)
        pre_2 = dot(rows_of(w_mid_cols, own_start, half), act_1, 0, 0) + dot(rows_of(w_mid_cols, other_start, half), act_1_other, 0, 0)
        mean_2, inv_2 = stats(pre_2)
        act_2 = jnp.maximum((pre_2 - mean_2) * inv_2 * gain_2h + bias_2h, 0.0).astype(BF16)
        act_2_other = lax.ppermute(act_2, DATA_AXIS, pair_perm)

        pieces = 2
        piece = block // pieces
        span = width // pieces
        w_out_cols = jnp.concatenate([cols_of(w_out, k * span + dev * piece, piece) for k in range(pieces)], axis=1)
        pre_z = dot(rows_of(w_out_cols, own_start, half), act_2, 0, 0) + dot(rows_of(w_out_cols, other_start, half), act_2_other, 0, 0)
        mean_z, inv_z = stats(pre_z)

        loss_part = 0.0
        grad_c_own, grad_z_own = [], []
        for k in range(pieces):
            pre_k, mean_k, inv_k = (v[k * piece:(k + 1) * piece] for v in (pre_z, mean_z, inv_z))
            if k:
                pre_k, grad_z_own[-1] = barrier((pre_k, grad_z_own[-1]))
            zh_a = (pre_k - mean_k) * inv_k
            corr_mat = dot(zh_a.astype(BF16), emb_b_all, 1, 0) / row_count
            feature = lax.broadcasted_iota(jnp.int32, corr_mat.shape, 0) + (k * span + dev * piece)
            on_diag = feature == lax.broadcasted_iota(jnp.int32, corr_mat.shape, 1)
            loss_k = jnp.sum(jnp.where(on_diag, jnp.square(1.0 - corr_mat), off_weight * jnp.square(corr_mat)))
            grad_c = jnp.where(on_diag, -2.0 * (1.0 - corr_mat), 2.0 * off_weight * corr_mat).astype(BF16)
            grad_z = norm_back(dot(grad_c, emb_b_all, 1, 1) / row_count, zh_a, inv_k).astype(BF16)
            loss_k, grad_z = barrier((loss_k, grad_z))
            loss_part = loss_part + loss_k
            grad_z_own.append(grad_z)
            grad_c_own.append(grad_c)
        grad_c_own[0], grad_c_own[1], grad_z_own[1] = barrier((grad_c_own[0], grad_c_own[1], grad_z_own[1]))
        grad_z_all = [gather(part) for part in grad_z_own]
        grad_c_all = [gather(part) for part in grad_c_own]

        w_out_rows = rows_of(w_out, own_start, half)
        out_own, grad_act_2 = [], None
        for k in range(pieces):
            grad_z_k = grad_z_all[k]
            if k:
                grad_z_k, grad_act_2 = barrier((grad_z_k, grad_act_2))
            part = dot(act_2, grad_z_k, 1, 1)
            part, grad_z_k = barrier((part, grad_z_k))
            out_own.append(part)
            part = dot(w_out_rows[:, k * span:(k + 1) * span], grad_z_k, 1, 0)
            grad_act_2 = part if grad_act_2 is None else grad_act_2 + part
        out_other = [lax.ppermute(part, DATA_AXIS, pair_perm) for part in out_own]
        places = [k * span for k in range(pieces)]
        grad_w_out = place_rows(None, out_own, places, own_start, width, width)
        grad_w_out = place_rows(grad_w_out, out_other, places, other_start, width, width)
        normed_2 = (pre_2 - mean_2) * inv_2
        grad_pre_2 = jnp.where(normed_2 * gain_2h + bias_2h > 0.0, grad_act_2, 0.0)
        grad_u_2, affine_2 = affine_back(grad_pre_2, normed_2, inv_2, gain_2h)
        grad_u_2_other = lax.ppermute(grad_u_2, DATA_AXIS, pair_perm)

        emb_parts = [dot(emb_b, part, 1, 1) / row_count for part in grad_c_all]
        *emb_parts, grad_u_2_other = barrier((*emb_parts, grad_u_2_other))
        grad_emb = place_rows(None, emb_parts, places, 0, emb_b.shape[0], width)

        part_start = chip * block
        w_mid_rows = rows_of(w_mid, own_start + part_start, block)
        normed_1 = (rows_of(pre_1, part_start, block) - rows_of(mean_1, part_start, block)) * rows_of(inv_1, part_start, block)
        gain_1p, bias_1p = rows_of(gain_1h, part_start, block), rows_of(bias_1h, part_start, block)
        grad_act_1 = dot(cols_of(w_mid_rows, own_start, half), grad_u_2, 1, 0) + dot(cols_of(w_mid_rows, other_start, half), grad_u_2_other, 1, 0)
        grad_pre_1 = jnp.where(normed_1 * gain_1p + bias_1p > 0.0, grad_act_1, 0.0)
        grad_u_1, affine_1 = affine_back(grad_pre_1, normed_1, rows_of(inv_1, part_start, block), gain_1p)
        grad_w_in_part = with_layout_constraint(dot(feat_all, grad_u_1, 0, 1), Layout(major_to_minor=(0, 1)))
        grad_w_in_parts = lax.all_gather(grad_w_in_part, DATA_AXIS)
        grad_w_in = join_columns(grad_w_in_parts, lambda i: (i % 2) * chips + i // 2)

        act_1, grad_w_in_part = barrier((act_1, grad_w_in_part))
        mid_own = [dot(act_1, grad_u_2, 1, 1), dot(act_1, grad_u_2_other, 1, 1)]
        mid_other = [lax.ppermute(part, DATA_AXIS, pair_perm) for part in mid_own]
        grad_w_mid = place_rows(None, mid_own, [own_start, other_start], own_start, width, width)
        grad_w_mid = place_rows(grad_w_mid, mid_other, [other_start, own_start], other_start, width, width)

        small = jnp.concatenate([affine_1, rows_of(affine_2, part_start, block)], axis=1).T
        small = jnp.concatenate([small, jnp.full((1, block), loss_part)], axis=0)
        small_all = lax.all_gather(small, DATA_AXIS)
        vectors = small_all.reshape(chips, 2, 5, block).transpose(2, 1, 0, 3).reshape(5, width)
        loss_value = jnp.sum(small_all[:, 4, 0])
        return (loss_value, grad_emb, grad_w_in, grad_w_mid, grad_w_out, vectors[0], vectors[1], vectors[2], vectors[3])

    return jax.shard_map(local_step, mesh=mesh, in_specs=(row_part, row_part) + (replicated,) * 11, out_specs=(replicated, row_part) + (replicated,) * 7, check_vma=False)
```

```python
import jax
import jax.numpy as jnp
from jax import lax
from jax.experimental import pallas as pl
from jax.experimental.layout import Layout, with_layout_constraint
from jax.experimental.pallas import tpu as pltpu
from jax.sharding import PartitionSpec as P

NORM_EPS = 1e-5
DATA_AXIS = "data"
F32 = jnp.float32
BF16 = jnp.bfloat16


barrier = lax.optimization_barrier


def dot(left_op, right_op, left_dim, right_dim):
    return lax.dot_general(left_op, right_op, (((left_dim,), (right_dim,)), ((), ())), preferred_element_type=F32)


def place_rows(buffer, pieces, starts, row_start, total_rows, total_cols, step=256):
    rows = pieces[0].shape[0]
    count = len(pieces)

    def kernel(where_ref, *refs):
        out_ref = refs[-1]
        for index in range(count):
            size = pieces[index].shape[1]
            if isinstance(starts[index], int):
                out_ref[:, starts[index]:starts[index] + size] = refs[index][...]
            else:
                out_ref[:, pl.ds(pl.multiple_of(where_ref[1 + index] * 128, 128), size)] = refs[index][...]

    where = jnp.stack([jnp.asarray(row_start // step, jnp.int32)] + [jnp.asarray(s // 128, jnp.int32) for s in starts])
    in_specs = [pl.BlockSpec((step, piece.shape[1]), lambda i, where_ref: (i, 0)) for piece in pieces]
    operands = list(pieces)
    aliases = {}
    if buffer is not None:
        in_specs.append(pl.BlockSpec(memory_space=pl.ANY))
        operands.append(buffer)
        aliases = {1 + count: 0}
    return pl.pallas_call(
        kernel,
        out_shape=jax.ShapeDtypeStruct((total_rows, total_cols), F32),
        grid_spec=pltpu.PrefetchScalarGridSpec(
            num_scalar_prefetch=1,
            grid=(rows // step,),
            in_specs=in_specs,
            out_specs=pl.BlockSpec((step, total_cols), lambda i, where_ref: (where_ref[0] + i, 0)),
        ),
        input_output_aliases=aliases,
        cost_estimate=pl.CostEstimate(flops=4 * 10**9, bytes_accessed=8 * rows * total_cols, transcendentals=0),
        compiler_params=pltpu.CompilerParams(vmem_limit_bytes=40 * 2**20),
    )(where, *operands)


def join_columns(parts, rows, order, step=256):
    count, _, cols = parts.shape

    def kernel(in_ref, out_ref):
        for i in range(count):
            out_ref[:, order(i) * cols:(order(i) + 1) * cols] = in_ref[i]

    return pl.pallas_call(
        kernel,
        out_shape=jax.ShapeDtypeStruct((rows, count * cols), F32),
        grid=(rows // step,),
        in_specs=[pl.BlockSpec((count, step, cols), lambda i: (0, i, 0))],
        out_specs=pl.BlockSpec((step, count * cols), lambda i: (i, 0)),
        cost_estimate=pl.CostEstimate(flops=4 * 10**9, bytes_accessed=8 * parts.size, transcendentals=0),
        compiler_params=pltpu.CompilerParams(vmem_limit_bytes=40 * 2**20),
    )(parts)


def split_columns(array, core, blocks, step=256):
    width = array.shape[1]
    half, piece = width // 2, width // blocks // 2

    def kernel(core_ref, in_ref, first_ref, second_ref):
        for i in range(blocks):
            low = 2 * i * piece
            first_ref[:, i * piece:(i + 1) * piece] = in_ref[:, low:low + piece]
            second_ref[:, i * piece:(i + 1) * piece] = in_ref[:, low + piece:low + 2 * piece]

    out_spec = pl.BlockSpec((step, half), lambda i, core_ref: (i, 0))
    return pl.pallas_call(
        kernel,
        out_shape=[jax.ShapeDtypeStruct((half, half), array.dtype)] * 2,
        grid_spec=pltpu.PrefetchScalarGridSpec(
            num_scalar_prefetch=1,
            grid=(half // step,),
            in_specs=[pl.BlockSpec((step, width), lambda i, core_ref: (core_ref[0] * (half // step) + i, 0))],
            out_specs=[out_spec, out_spec],
        ),
        cost_estimate=pl.CostEstimate(flops=2 * 10**9, bytes_accessed=4 * half * width, transcendentals=0),
    )(jnp.asarray(core, jnp.int32)[None], array)


def place_pieces(buffer, first, second, core, blocks, step=256):
    half, width = first.shape[0], 2 * first.shape[1]
    piece = width // blocks // 2
    per_block = second.shape[1] // step

    def kernel(core_ref, first_ref, second_ref, *rest):
        out_ref = rest[-1]
        for i in range(blocks):
            low = 2 * i * piece
            out_ref[:, low:low + piece] = first_ref[:, i * piece:(i + 1) * piece]
            out_ref[:, low + piece:low + 2 * piece] = second_ref[0, :, i * piece:(i + 1) * piece]

    in_specs = [
        pl.BlockSpec((step, half), lambda i, core_ref: (i, 0)),
        pl.BlockSpec((1, step, half), lambda i, core_ref: (2 * (i // per_block) + core_ref[0], i % per_block, 0)),
    ]
    operands = [first, second]
    aliases = {}
    if buffer is not None:
        in_specs.append(pl.BlockSpec(memory_space=pl.ANY))
        operands.append(buffer)
        aliases = {3: 0}
    return pl.pallas_call(
        kernel,
        out_shape=jax.ShapeDtypeStruct((width, width), F32),
        grid_spec=pltpu.PrefetchScalarGridSpec(
            num_scalar_prefetch=1,
            grid=(half // step,),
            in_specs=in_specs,
            out_specs=pl.BlockSpec((step, width), lambda i, core_ref: (core_ref[0] * (half // step) + i, 0)),
        ),
        input_output_aliases=aliases,
        cost_estimate=pl.CostEstimate(flops=4 * 10**9, bytes_accessed=8 * half * width, transcendentals=0),
        compiler_params=pltpu.CompilerParams(vmem_limit_bytes=40 * 2**20),
    )(jnp.asarray(core, jnp.int32)[None], *operands)


def solution(mesh):
    shards = mesh.shape[DATA_AXIS]
    chips = shards // 2
    row_part = P(DATA_AXIS, None)
    replicated = P()
    pair_groups = [[2 * i, 2 * i + 1] for i in range(chips)]
    pair_perm = [(i, i ^ 1) for i in range(shards)]

    def local_step(feat_a, feat_b, w_in, w_mid, w_out, t_in, t_mid, t_out, gain_1, bias_1, gain_2, bias_2, off_weight):
        row_count = feat_a.shape[0] * shards
        width = w_mid.shape[0]
        half = width // 2
        block = width // shards
        dev = lax.axis_index(DATA_AXIS)
        core = dev % 2
        chip = dev // 2
        own_start = core * half
        other_start = (1 - core) * half

        def rows_of(array, start, size):
            return lax.dynamic_slice_in_dim(array, start, size, 0)

        def cols_of(array, start, size):
            return lax.dynamic_slice_in_dim(array, start, size, 1)

        def gather(array):
            return lax.all_gather(array, DATA_AXIS, axis=0, tiled=True)

        def pair_gather(array):
            return lax.all_gather(array, DATA_AXIS, axis=0, tiled=True, axis_index_groups=pair_groups)

        def norm_rows(pre):
            sums = lax.all_gather(jnp.stack([jnp.sum(pre, axis=0), jnp.sum(pre * pre, axis=0)]), DATA_AXIS)
            means = jnp.sum(sums, axis=0) / row_count
            inv = lax.rsqrt(jnp.maximum(means[1] - means[0] * means[0], 0.0) + NORM_EPS)
            return (pre - means[0]) * inv

        def teacher_layer(layer_in, weight, gain_vec, bias_vec):
            normed = norm_rows(jnp.dot(layer_in, weight, preferred_element_type=F32))
            return jnp.maximum(normed * gain_vec + bias_vec, 0.0).astype(BF16)

        def stats(pre):
            mean = jnp.sum(pre, axis=1, keepdims=True) / row_count
            square = jnp.sum(pre * pre, axis=1, keepdims=True) / row_count
            return mean, lax.rsqrt(jnp.maximum(square - mean * mean, 0.0) + NORM_EPS)

        def norm_back(grad_n, normed, inv_std):
            mean_g = jnp.sum(grad_n, axis=1, keepdims=True) / row_count
            mean_gn = jnp.sum(grad_n * normed, axis=1, keepdims=True) / row_count
            return (grad_n - mean_g - normed * mean_gn) * inv_std

        def affine_back(grad_pre, normed, inv_std, gain_col):
            sum_gn = jnp.sum(grad_pre * normed, axis=1, keepdims=True)
            sum_g = jnp.sum(grad_pre, axis=1, keepdims=True)
            grad_u = (grad_pre - sum_g / row_count - normed * (sum_gn / row_count)) * (gain_col * inv_std)
            return grad_u.astype(BF16), jnp.concatenate([sum_gn, sum_g], axis=1)

        feat_all = gather(feat_a)
        teach_1 = teacher_layer(feat_b, t_in, gain_1, bias_1)
        teach_2 = teacher_layer(teach_1, t_mid, gain_2, bias_2)
        emb_b = norm_rows(jnp.dot(teach_2, t_out, preferred_element_type=F32)).astype(BF16)
        emb_b_all = gather(emb_b)

        gain_1h, bias_1h, gain_2h, bias_2h = (rows_of(v[:, None], own_start, half) for v in (gain_1, bias_1, gain_2, bias_2))

        pre_1 = dot(cols_of(w_in, own_start, half), feat_all, 0, 1)
        mean_1, inv_1 = stats(pre_1)
        act_1 = jnp.maximum((pre_1 - mean_1) * inv_1 * gain_1h + bias_1h, 0.0).astype(BF16)
        act_1_other = lax.ppermute(act_1, DATA_AXIS, pair_perm)

        w_mid_cols = cols_of(w_mid, own_start, half)
        pre_2 = dot(rows_of(w_mid_cols, own_start, half), act_1, 0, 0) + dot(rows_of(w_mid_cols, other_start, half), act_1_other, 0, 0)
        mean_2, inv_2 = stats(pre_2)
        act_2 = jnp.maximum((pre_2 - mean_2) * inv_2 * gain_2h + bias_2h, 0.0).astype(BF16)
        act_2_other = lax.ppermute(act_2, DATA_AXIS, pair_perm)

        pieces = 2
        piece = block // pieces
        w_out_cols = cols_of(w_out, dev * block, block)
        w_out_other = rows_of(w_out_cols, other_start, half)
        pre_z_own = dot(rows_of(w_out_cols, own_start, half), act_2, 0, 0)
        w_out_pieces = list(split_columns(w_out, core, shards))
        act_2_other, w_out_pieces[0] = barrier((act_2_other, w_out_pieces[0]))

        loss_part = 0.0
        grad_c_own, grad_z_own = [], []
        for k in range(pieces):
            w_k, pre_k = w_out_other[:, k * piece:(k + 1) * piece], pre_z_own[k * piece:(k + 1) * piece]
            if k:
                w_k, pre_k, grad_z_own[-1] = barrier((w_k, pre_k, grad_z_own[-1]))
            pre_k = pre_k + dot(w_k, act_2_other, 0, 0)
            mean_k, inv_k = stats(pre_k)
            zh_a = (pre_k - mean_k) * inv_k
            corr_mat = dot(zh_a.astype(BF16), emb_b_all, 1, 0) / row_count
            feature = lax.broadcasted_iota(jnp.int32, corr_mat.shape, 0) + (dev * block + k * piece)
            on_diag = feature == lax.broadcasted_iota(jnp.int32, corr_mat.shape, 1)
            loss_k = jnp.sum(jnp.where(on_diag, jnp.square(1.0 - corr_mat), off_weight * jnp.square(corr_mat)))
            grad_c = jnp.where(on_diag, -2.0 * (1.0 - corr_mat), 2.0 * off_weight * corr_mat).astype(BF16)
            grad_z = norm_back(dot(grad_c, emb_b_all, 1, 1) / row_count, zh_a, inv_k).astype(BF16)
            loss_k, grad_z = barrier((loss_k, grad_z))
            loss_part = loss_part + loss_k
            grad_z_own.append(grad_z)
            grad_c_own.append(grad_c)
        grad_c_own[0], grad_c_own[1], grad_z_own[1] = barrier((grad_c_own[0], grad_c_own[1], grad_z_own[1]))
        grad_z_all = [gather(part) for part in grad_z_own]
        grad_c_all = gather(jnp.concatenate(grad_c_own, axis=0))

        part_start = chip * block
        out_first = dot(act_2, grad_z_all[0], 1, 1)
        out_first, grad_z_first = barrier((out_first, grad_z_all[0]))
        grad_act_2 = dot(w_out_pieces[0], grad_z_first, 1, 0)
        grad_act_2, grad_z_second = barrier((grad_act_2, grad_z_all[1]))
        out_second = dot(rows_of(act_2, part_start, block), grad_z_second, 1, 1)
        out_second, grad_z_second = barrier((out_second, grad_z_second))
        grad_act_2 = grad_act_2 + dot(w_out_pieces[1], grad_z_second, 1, 0)
        out_first_other = lax.ppermute(out_first, DATA_AXIS, pair_perm)
        out_second_all = lax.all_gather(out_second, DATA_AXIS)
        grad_w_out = place_pieces(None, out_first, out_second_all, core, shards)
        grad_w_out = place_pieces(grad_w_out, out_first_other, out_second_all, 1 - core, shards)
        normed_2 = (pre_2 - mean_2) * inv_2
        grad_pre_2 = jnp.where(normed_2 * gain_2h + bias_2h > 0.0, grad_act_2, 0.0)
        grad_u_2, affine_2 = affine_back(grad_pre_2, normed_2, inv_2, gain_2h)
        grad_u_2_other = lax.ppermute(grad_u_2, DATA_AXIS, pair_perm)

        grad_emb = dot(emb_b, grad_c_all, 1, 1) / row_count
        grad_emb, grad_u_2_other = barrier((grad_emb, grad_u_2_other))

        w_mid_rows = rows_of(w_mid, own_start + part_start, block)
        normed_1 = (rows_of(pre_1, part_start, block) - rows_of(mean_1, part_start, block)) * rows_of(inv_1, part_start, block)
        gain_1p, bias_1p = rows_of(gain_1h, part_start, block), rows_of(bias_1h, part_start, block)
        grad_act_1 = dot(cols_of(w_mid_rows, own_start, half), grad_u_2, 1, 0) + dot(cols_of(w_mid_rows, other_start, half), grad_u_2_other, 1, 0)
        grad_pre_1 = jnp.where(normed_1 * gain_1p + bias_1p > 0.0, grad_act_1, 0.0)
        grad_u_1, affine_1 = affine_back(grad_pre_1, normed_1, rows_of(inv_1, part_start, block), gain_1p)
        grad_w_in_part = with_layout_constraint(dot(feat_all, grad_u_1, 0, 1), Layout(major_to_minor=(0, 1)))
        small = jnp.concatenate([affine_1, rows_of(affine_2, part_start, block)], axis=1).T
        small = jnp.concatenate([small, jnp.full((4, block), loss_part)], axis=0)
        gathered = lax.all_gather(jnp.concatenate([grad_w_in_part, small], axis=0), DATA_AXIS)
        features = grad_w_in_part.shape[0]
        grad_w_in = join_columns(gathered, features, lambda i: (i % 2) * chips + i // 2)
        small_all = gathered[:, features:features + 5]
        vectors = small_all.reshape(chips, 2, 5, block).transpose(2, 1, 0, 3).reshape(5, width)
        loss_value = jnp.sum(small_all[:, 4, 0])

        act_1, grad_w_in_part = barrier((act_1, grad_w_in_part))
        mid_own = [dot(act_1, grad_u_2, 1, 1), dot(act_1, grad_u_2_other, 1, 1)]
        mid_other = [lax.ppermute(part, DATA_AXIS, pair_perm) for part in mid_own]
        grad_w_mid = place_rows(None, mid_own, [own_start, other_start], own_start, width, width)
        mid_other[0], mid_other[1], grad_w_out = barrier((mid_other[0], mid_other[1], grad_w_out))
        grad_w_mid = place_rows(grad_w_mid, mid_other, [other_start, own_start], other_start, width, width)

        return (loss_value, grad_emb, grad_w_in, grad_w_mid, grad_w_out, vectors[0], vectors[1], vectors[2], vectors[3])

    return jax.shard_map(local_step, mesh=mesh, in_specs=(row_part, row_part) + (replicated,) * 11, out_specs=(replicated, row_part) + (replicated,) * 7, check_vma=False)
```

```python
import jax
import jax.numpy as jnp
from jax import lax
from jax.experimental import pallas as pl
from jax.experimental.layout import Layout, with_layout_constraint
from jax.experimental.pallas import tpu as pltpu
from jax.sharding import PartitionSpec as P

NORM_EPS = 1e-5
DATA_AXIS = "data"
F32 = jnp.float32
BF16 = jnp.bfloat16


barrier = lax.optimization_barrier


def dot(left_op, right_op, left_dim, right_dim):
    return lax.dot_general(left_op, right_op, (((left_dim,), (right_dim,)), ((), ())), preferred_element_type=F32)


def place_rows(buffer, pieces, gathered, core, other_core, total, step=256):
    half = total // 2
    part = gathered.shape[2] // 2
    per_block = gathered.shape[1] // step

    def kernel(core_ref, own_ref, other_ref, gathered_ref, *rest):
        out_ref = rest[-1]
        for k, piece_ref in ((0, own_ref), (1, other_ref)):
            low = core_ref[k] * half
            out_ref[:, pl.ds(pl.multiple_of(low, 128), part)] = gathered_ref[0, :, k * part:(k + 1) * part]
            out_ref[:, pl.ds(pl.multiple_of(low + part, 128), half - part)] = piece_ref[...]

    cores = jnp.stack([jnp.asarray(core, jnp.int32), jnp.asarray(other_core, jnp.int32)])
    in_specs = [pl.BlockSpec((step, half - part), lambda i, core_ref: (i, 0))] * 2
    in_specs.append(pl.BlockSpec((1, step, 2 * part), lambda i, core_ref: (2 * (i // per_block) + core_ref[0], i % per_block, 0)))
    operands = [*pieces, gathered]
    aliases = {}
    if buffer is not None:
        in_specs.append(pl.BlockSpec(memory_space=pl.ANY))
        operands.append(buffer)
        aliases = {4: 0}
    return pl.pallas_call(
        kernel,
        out_shape=jax.ShapeDtypeStruct((total, total), F32),
        grid_spec=pltpu.PrefetchScalarGridSpec(
            num_scalar_prefetch=1,
            grid=(half // step,),
            in_specs=in_specs,
            out_specs=pl.BlockSpec((step, total), lambda i, core_ref: (core_ref[0] * (half // step) + i, 0)),
        ),
        input_output_aliases=aliases,
        cost_estimate=pl.CostEstimate(flops=4 * 10**9, bytes_accessed=8 * half * total, transcendentals=0),
        compiler_params=pltpu.CompilerParams(vmem_limit_bytes=40 * 2**20),
    )(cores, *operands)


def join_columns(parts, rows, order, step=256):
    count, _, cols = parts.shape

    def kernel(in_ref, out_ref):
        for i in range(count):
            out_ref[:, order(i) * cols:(order(i) + 1) * cols] = in_ref[i]

    return pl.pallas_call(
        kernel,
        out_shape=jax.ShapeDtypeStruct((rows, count * cols), F32),
        grid=(rows // step,),
        in_specs=[pl.BlockSpec((count, step, cols), lambda i: (0, i, 0))],
        out_specs=pl.BlockSpec((step, count * cols), lambda i: (i, 0)),
        cost_estimate=pl.CostEstimate(flops=4 * 10**9, bytes_accessed=8 * parts.size, transcendentals=0),
        compiler_params=pltpu.CompilerParams(vmem_limit_bytes=40 * 2**20),
    )(parts)


def split_columns(array, core, blocks, step=256):
    width = array.shape[1]
    half, piece = width // 2, width // blocks // 2

    def kernel(core_ref, in_ref, first_ref, second_ref):
        for i in range(blocks):
            low = 2 * i * piece
            first_ref[:, i * piece:(i + 1) * piece] = in_ref[:, low:low + piece]
            second_ref[:, i * piece:(i + 1) * piece] = in_ref[:, low + piece:low + 2 * piece]

    out_spec = pl.BlockSpec((step, half), lambda i, core_ref: (i, 0))
    return pl.pallas_call(
        kernel,
        out_shape=[jax.ShapeDtypeStruct((half, half), array.dtype)] * 2,
        grid_spec=pltpu.PrefetchScalarGridSpec(
            num_scalar_prefetch=1,
            grid=(half // step,),
            in_specs=[pl.BlockSpec((step, width), lambda i, core_ref: (core_ref[0] * (half // step) + i, 0))],
            out_specs=[out_spec, out_spec],
        ),
        cost_estimate=pl.CostEstimate(flops=2 * 10**9, bytes_accessed=4 * half * width, transcendentals=0),
    )(jnp.asarray(core, jnp.int32)[None], array)


def place_pieces(buffer, first, second, core, blocks, step=256):
    half, width = first.shape[0], 2 * first.shape[1]
    piece = width // blocks // 2
    per_block = second.shape[1] // step

    def kernel(core_ref, first_ref, second_ref, *rest):
        out_ref = rest[-1]
        for i in range(blocks):
            low = 2 * i * piece
            out_ref[:, low:low + piece] = first_ref[:, i * piece:(i + 1) * piece]
            out_ref[:, low + piece:low + 2 * piece] = second_ref[0, :, i * piece:(i + 1) * piece]

    in_specs = [
        pl.BlockSpec((step, half), lambda i, core_ref: (i, 0)),
        pl.BlockSpec((1, step, half), lambda i, core_ref: (2 * (i // per_block) + core_ref[0], i % per_block, 0)),
    ]
    operands = [first, second]
    aliases = {}
    if buffer is not None:
        in_specs.append(pl.BlockSpec(memory_space=pl.ANY))
        operands.append(buffer)
        aliases = {3: 0}
    return pl.pallas_call(
        kernel,
        out_shape=jax.ShapeDtypeStruct((width, width), F32),
        grid_spec=pltpu.PrefetchScalarGridSpec(
            num_scalar_prefetch=1,
            grid=(half // step,),
            in_specs=in_specs,
            out_specs=pl.BlockSpec((step, width), lambda i, core_ref: (core_ref[0] * (half // step) + i, 0)),
        ),
        input_output_aliases=aliases,
        cost_estimate=pl.CostEstimate(flops=4 * 10**9, bytes_accessed=8 * half * width, transcendentals=0),
        compiler_params=pltpu.CompilerParams(vmem_limit_bytes=40 * 2**20),
    )(jnp.asarray(core, jnp.int32)[None], *operands)


def solution(mesh):
    shards = mesh.shape[DATA_AXIS]
    chips = shards // 2
    row_part = P(DATA_AXIS, None)
    replicated = P()
    pair_groups = [[2 * i, 2 * i + 1] for i in range(chips)]
    pair_perm = [(i, i ^ 1) for i in range(shards)]

    def local_step(feat_a, feat_b, w_in, w_mid, w_out, t_in, t_mid, t_out, gain_1, bias_1, gain_2, bias_2, off_weight):
        row_count = feat_a.shape[0] * shards
        width = w_mid.shape[0]
        half = width // 2
        block = width // shards
        dev = lax.axis_index(DATA_AXIS)
        core = dev % 2
        chip = dev // 2
        own_start = core * half
        other_start = (1 - core) * half

        def rows_of(array, start, size):
            return lax.dynamic_slice_in_dim(array, start, size, 0)

        def cols_of(array, start, size):
            return lax.dynamic_slice_in_dim(array, start, size, 1)

        def gather(array):
            return lax.all_gather(array, DATA_AXIS, axis=0, tiled=True)

        def pair_gather(array):
            return lax.all_gather(array, DATA_AXIS, axis=0, tiled=True, axis_index_groups=pair_groups)

        def norm_rows(pre):
            sums = lax.all_gather(jnp.stack([jnp.sum(pre, axis=0), jnp.sum(pre * pre, axis=0)]), DATA_AXIS)
            means = jnp.sum(sums, axis=0) / row_count
            inv = lax.rsqrt(jnp.maximum(means[1] - means[0] * means[0], 0.0) + NORM_EPS)
            return (pre - means[0]) * inv

        def teacher_layer(layer_in, weight, gain_vec, bias_vec):
            normed = norm_rows(jnp.dot(layer_in, weight, preferred_element_type=F32))
            return jnp.maximum(normed * gain_vec + bias_vec, 0.0).astype(BF16)

        def stats(pre):
            mean = jnp.sum(pre, axis=1, keepdims=True) / row_count
            square = jnp.sum(pre * pre, axis=1, keepdims=True) / row_count
            return mean, lax.rsqrt(jnp.maximum(square - mean * mean, 0.0) + NORM_EPS)

        def norm_back(grad_n, normed, inv_std):
            mean_g = jnp.sum(grad_n, axis=1, keepdims=True) / row_count
            mean_gn = jnp.sum(grad_n * normed, axis=1, keepdims=True) / row_count
            return (grad_n - mean_g - normed * mean_gn) * inv_std

        def affine_back(grad_pre, normed, inv_std, gain_col):
            sum_gn = jnp.sum(grad_pre * normed, axis=1, keepdims=True)
            sum_g = jnp.sum(grad_pre, axis=1, keepdims=True)
            grad_u = (grad_pre - sum_g / row_count - normed * (sum_gn / row_count)) * (gain_col * inv_std)
            return grad_u.astype(BF16), jnp.concatenate([sum_gn, sum_g], axis=1)

        feat_all = gather(feat_a)
        teach_1 = teacher_layer(feat_b, t_in, gain_1, bias_1)
        teach_2 = teacher_layer(teach_1, t_mid, gain_2, bias_2)
        emb_b = norm_rows(jnp.dot(teach_2, t_out, preferred_element_type=F32)).astype(BF16)
        emb_b_all = gather(emb_b)

        gain_1h, bias_1h, gain_2h, bias_2h = (rows_of(v[:, None], own_start, half) for v in (gain_1, bias_1, gain_2, bias_2))

        pre_1 = dot(cols_of(w_in, own_start, half), feat_all, 0, 1)
        mean_1, inv_1 = stats(pre_1)
        act_1 = jnp.maximum((pre_1 - mean_1) * inv_1 * gain_1h + bias_1h, 0.0).astype(BF16)
        act_1_other = lax.ppermute(act_1, DATA_AXIS, pair_perm)

        w_mid_cols = cols_of(w_mid, own_start, half)
        pre_2 = dot(rows_of(w_mid_cols, own_start, half), act_1, 0, 0) + dot(rows_of(w_mid_cols, other_start, half), act_1_other, 0, 0)
        mean_2, inv_2 = stats(pre_2)
        act_2 = jnp.maximum((pre_2 - mean_2) * inv_2 * gain_2h + bias_2h, 0.0).astype(BF16)
        act_2_other = lax.ppermute(act_2, DATA_AXIS, pair_perm)

        pieces = 2
        piece = block // pieces
        w_out_cols = cols_of(w_out, dev * block, block)
        w_out_other = rows_of(w_out_cols, other_start, half)
        pre_z_own = dot(rows_of(w_out_cols, own_start, half), act_2, 0, 0)
        w_out_pieces = list(split_columns(w_out, core, shards))
        act_2_other, w_out_pieces[0] = barrier((act_2_other, w_out_pieces[0]))

        loss_part = 0.0
        grad_c_own, grad_z_own = [], []
        for k in range(pieces):
            w_k, pre_k = w_out_other[:, k * piece:(k + 1) * piece], pre_z_own[k * piece:(k + 1) * piece]
            if k:
                w_k, pre_k, grad_z_own[-1] = barrier((w_k, pre_k, grad_z_own[-1]))
            pre_k = pre_k + dot(w_k, act_2_other, 0, 0)
            mean_k, inv_k = stats(pre_k)
            zh_a = (pre_k - mean_k) * inv_k
            corr_mat = dot(zh_a.astype(BF16), emb_b_all, 1, 0) / row_count
            feature = lax.broadcasted_iota(jnp.int32, corr_mat.shape, 0) + (dev * block + k * piece)
            on_diag = feature == lax.broadcasted_iota(jnp.int32, corr_mat.shape, 1)
            loss_k = jnp.sum(jnp.where(on_diag, jnp.square(1.0 - corr_mat), off_weight * jnp.square(corr_mat)))
            grad_c = jnp.where(on_diag, -2.0 * (1.0 - corr_mat), 2.0 * off_weight * corr_mat).astype(BF16)
            grad_z = norm_back(dot(grad_c, emb_b_all, 1, 1) / row_count, zh_a, inv_k).astype(BF16)
            loss_k, grad_z = barrier((loss_k, grad_z))
            loss_part = loss_part + loss_k
            grad_z_own.append(grad_z)
            grad_c_own.append(grad_c)
        grad_c_own[0], grad_c_own[1], grad_z_own[1] = barrier((grad_c_own[0], grad_c_own[1], grad_z_own[1]))
        grad_z_all = [gather(part) for part in grad_z_own]
        grad_c_all = gather(jnp.concatenate(grad_c_own, axis=0))

        part_start = chip * block
        out_first = dot(act_2, grad_z_all[0], 1, 1)
        out_first, grad_z_first = barrier((out_first, grad_z_all[0]))
        grad_act_2 = dot(w_out_pieces[0], grad_z_first, 1, 0)
        grad_act_2, grad_z_second = barrier((grad_act_2, grad_z_all[1]))
        out_second = dot(rows_of(act_2, part_start, block), grad_z_second, 1, 1)
        out_second, grad_z_second = barrier((out_second, grad_z_second))
        grad_act_2 = grad_act_2 + dot(w_out_pieces[1], grad_z_second, 1, 0)
        out_first_other = lax.ppermute(out_first, DATA_AXIS, pair_perm)
        out_second_all = lax.all_gather(out_second, DATA_AXIS)
        grad_w_out = place_pieces(None, out_first, out_second_all, core, shards)
        grad_w_out = place_pieces(grad_w_out, out_first_other, out_second_all, 1 - core, shards)
        normed_2 = (pre_2 - mean_2) * inv_2
        grad_pre_2 = jnp.where(normed_2 * gain_2h + bias_2h > 0.0, grad_act_2, 0.0)
        grad_u_2, affine_2 = affine_back(grad_pre_2, normed_2, inv_2, gain_2h)
        grad_u_2_other = lax.ppermute(grad_u_2, DATA_AXIS, pair_perm)

        grad_emb = dot(emb_b, grad_c_all, 1, 1) / row_count
        grad_emb, grad_u_2_other = barrier((grad_emb, grad_u_2_other))

        act_1_part = rows_of(act_1, part_start, block)
        mid_part = jnp.concatenate([dot(act_1_part, grad_u_2[:block], 1, 1), dot(act_1_part, grad_u_2_other[:block], 1, 1)], axis=1)
        mid_part = with_layout_constraint(mid_part, Layout(major_to_minor=(0, 1)))
        mid_gathered = lax.all_gather(mid_part, DATA_AXIS)
        mid_part, grad_u_2_other = barrier((mid_part, grad_u_2_other))

        w_mid_rows = rows_of(w_mid, own_start + part_start, block)
        normed_1 = (rows_of(pre_1, part_start, block) - rows_of(mean_1, part_start, block)) * rows_of(inv_1, part_start, block)
        gain_1p, bias_1p = rows_of(gain_1h, part_start, block), rows_of(bias_1h, part_start, block)
        grad_act_1 = dot(cols_of(w_mid_rows, own_start, half), grad_u_2, 1, 0) + dot(cols_of(w_mid_rows, other_start, half), grad_u_2_other, 1, 0)
        grad_pre_1 = jnp.where(normed_1 * gain_1p + bias_1p > 0.0, grad_act_1, 0.0)
        grad_u_1, affine_1 = affine_back(grad_pre_1, normed_1, rows_of(inv_1, part_start, block), gain_1p)
        grad_w_in_part = with_layout_constraint(dot(feat_all, grad_u_1, 0, 1), Layout(major_to_minor=(0, 1)))
        small = jnp.concatenate([affine_1, rows_of(affine_2, part_start, block)], axis=1).T
        small = jnp.concatenate([small, jnp.full((4, block), loss_part)], axis=0)
        gathered = lax.all_gather(jnp.concatenate([grad_w_in_part, small], axis=0), DATA_AXIS)
        features = grad_w_in_part.shape[0]
        grad_w_in = join_columns(gathered, features, lambda i: (i % 2) * chips + i // 2)
        small_all = gathered[:, features:features + 5]
        vectors = small_all.reshape(chips, 2, 5, block).transpose(2, 1, 0, 3).reshape(5, width)
        loss_value = jnp.sum(small_all[:, 4, 0])

        act_1, grad_w_in_part = barrier((act_1, grad_w_in_part))
        mid_own = [dot(act_1, grad_u_2[block:], 1, 1), dot(act_1, grad_u_2_other[block:], 1, 1)]
        mid_other = [lax.ppermute(part, DATA_AXIS, pair_perm) for part in mid_own]
        grad_w_mid = place_rows(None, mid_own, mid_gathered, core, 1 - core, width)
        mid_other[0], mid_other[1], grad_w_out = barrier((mid_other[0], mid_other[1], grad_w_out))
        grad_w_mid = place_rows(grad_w_mid, mid_other, mid_gathered, 1 - core, core, width)

        return (loss_value, grad_emb, grad_w_in, grad_w_mid, grad_w_out, vectors[0], vectors[1], vectors[2], vectors[3])

    return jax.shard_map(local_step, mesh=mesh, in_specs=(row_part, row_part) + (replicated,) * 11, out_specs=(replicated, row_part) + (replicated,) * 7, check_vma=False)
```
